256 devices in a mesh: grp: 16 (over x, y_hi, core), rng: 16 (over z, y_lo).
Axes of the slice: x: 4, y: 4 (y_hi: 2, y_lo: 2; y = y_hi * 2 + y_lo), z: 8, core: 2. Of those that a mesh axis runs over, the one named last changes fastest.
Arguments:
- features: bfloat16 [65536, 1024], P(('grp', 'rng')), may hold values from -6 to 6
- query_weight: bfloat16 [1024, 1024], replicated
- key_weight: bfloat16 [1024, 1024], replicated
- value_weight: bfloat16 [1024, 1024], replicated, may hold values from -0.1875 to 0.1875
- out_weight: bfloat16 [1024, 1024], replicated, may hold values from -0.1875 to 0.1875
- band_reach: int32 [256], P(('grp', 'rng')), may hold values from 16 to 128, as said below
- long_peers: int32 [512, 6], P(('grp', 'rng')), may hold values from 0 to 15, as said below
- long_count: int32 [512], P(('grp', 'rng')), may hold values from 0 to 6, as said below
- send_tile: int32 [256, 16], P(('grp', 'rng')), may hold values from 0 to 3
Outputs:
- updated: bfloat16 [65536, 1024], P(('grp', 'rng'))
The draws below stay inside these ranges and needn't reach their ends.
Inputs may be any that keep to these rules, and one draw needn't show every extreme that they name: `band_reach`: some range has 128 in every draw. `long_peers`: the 6 entries of a query tile in region g are distinct regions other than g; only the first long_count entries are used. `long_count`: some query tile has 6 in every draw.
All inputs are finite; a program needn't handle non-finite values.
Results may differ from the reference program's by a relative error of at most 0.0064.
Values may be sent and summed in bfloat16 or wider, within the bound.
No kernel may reach another device: no remote copies, remote signals or barrier semaphores. Data moves between devices by JAX's collectives and lax.ppermute only.
A program may use at most 128 MiB of HBM per device.

```python
import jax
import jax.numpy as jnp
from jax import lax

D = 1024
HEADS = 16
TOK_DEV = 256
TILE = 128
PORTAL = 64
MAXLONG = 6
REGION = 4096
NODES = 65536
QTILES = 512
N_GRP = 16
N_RNG = 16


def projection_pair(key):
    key_part = jax.random.normal(jax.random.fold_in(key, 12), (D, D), jnp.float32) * D ** (-0.5)
    query_noise = jax.random.normal(jax.random.fold_in(key, 11), (D, D), jnp.float32)
    query_part = query_noise * (D // 8) ** (-0.5)
    return (query_part, key_part)


def draw_query_weight(key, part):
    return projection_pair(key)[0].astype(jnp.bfloat16)


def draw_key_weight(key, part):
    return projection_pair(key)[1].astype(jnp.bfloat16)


def draw_band_reach(key, part):
    device_total = NODES // TOK_DEV
    reaches = jax.random.randint(jax.random.fold_in(key, 21), (device_total,), TILE // 8, TILE + 1)
    chosen = jax.random.randint(jax.random.fold_in(key, 22), (), 0, device_total)
    return jnp.where(jnp.arange(device_total) == chosen, TILE, reaches).astype(jnp.int32)


def draw_long_count(key, part):
    device_total = NODES // TOK_DEV
    per_device = TOK_DEV // TILE
    heavy_ranges = jax.random.randint(jax.random.fold_in(key, 31), (device_total,), 0, 4) == 0
    chosen = jax.random.randint(jax.random.fold_in(key, 32), (), 0, device_total)
    heavy_ranges = heavy_ranges | (jnp.arange(device_total) == chosen)
    device_cap = jnp.where(heavy_ranges, MAXLONG, MAXLONG // 3)
    tile_cap = jnp.repeat(device_cap, per_device)
    counts = jax.random.randint(jax.random.fold_in(key, 33), (QTILES,), 0, 1 << 20) % (tile_cap + 1)
    counts = jnp.where(jnp.arange(QTILES) == chosen * per_device, MAXLONG, counts)
    return counts.astype(jnp.int32)


def draw_long_peers(key, part):
    regions = NODES // REGION
    ranking_keys = jax.random.randint(jax.random.fold_in(key, 41), (QTILES, regions - 1), 0, 1 << 20) * regions
    ranking_keys = ranking_keys + jnp.arange(regions - 1, dtype=jnp.int32)[None, :]
    ranking = jnp.argsort(ranking_keys, axis=1, stable=True)[:, :MAXLONG].astype(jnp.int32)
    home_region = jnp.arange(QTILES, dtype=jnp.int32) * TILE // REGION
    return jnp.where(ranking >= home_region[:, None], ranking + 1, ranking).astype(jnp.int32)


def touch_ends(result, stream_key, least, top_value):
    spot = [jax.random.randint(jax.random.fold_in(stream_key, axis), (), 0, length) for axis, length in enumerate(result.shape)]
    main_axis = result.shape.index(max(result.shape))
    next_to = spot[:main_axis] + [(spot[main_axis] + 1) % result.shape[main_axis]] + spot[main_axis + 1:]
    return result.at[tuple(spot)].set(least).at[tuple(next_to)].set(top_value)


def block_levels(key, extent, shards, smallest, high):
    def one(dim, shards_of):
        draws = jax.random.uniform(jax.random.fold_in(jax.random.fold_in(key, 6), dim), (shards_of,), jnp.float32, smallest / len(shards), high / len(shards))
        return jnp.repeat(jnp.exp(draws), extent[dim] // shards_of).reshape((-1,) + (1,) * (len(extent) - dim - 1))

    level = one(*shards[0])
    for cut in shards[1:]:
        level = level * one(*cut)
    return level


def bell_draw(rng, dims, spread, reach, cuts=(), held_as=jnp.bfloat16):
    values = jax.random.normal(rng, dims, jnp.float32) * spread
    if len(cuts) > 0:
        values = block_levels(rng, dims, cuts, -0.22, 0.18) * values
    return jnp.clip(values, min=-reach, max=reach).astype(held_as)


def setup_inputs(seed: int = 0) -> dict:
    streams_of = jax.random.split(jax.random.key(seed), 10)
    features = bell_draw(streams_of[0], (NODES, D), 1.0, 6.0, ((0, 256),))
    query_weight = draw_query_weight(jax.random.fold_in(streams_of[9], 71), 0)
    key_weight = draw_key_weight(jax.random.fold_in(streams_of[9], 71), 0)
    value_weight = bell_draw(streams_of[3], (D, D), D ** -0.5, 0.1875)
    out_weight = bell_draw(streams_of[4], (D, D), D ** -0.5, 0.1875)
    band_reach = draw_band_reach(jax.random.fold_in(streams_of[9], 71), 0)
    long_peers = draw_long_peers(jax.random.fold_in(streams_of[9], 71), 0)
    long_count = draw_long_count(jax.random.fold_in(streams_of[9], 71), 0)
    send_tile = touch_ends(jax.random.randint(streams_of[8], (N_GRP * N_RNG, N_GRP), 0, TOK_DEV // PORTAL), jax.random.fold_in(streams_of[8], 1), 0, (TOK_DEV // PORTAL) - 1).astype(jnp.int32)
    return {"features": features, "query_weight": query_weight, "key_weight": key_weight, "value_weight": value_weight, "out_weight": out_weight, "band_reach": band_reach, "long_peers": long_peers, "long_count": long_count, "send_tile": send_tile}


EPSILON = 1e-06

def reference(features, query_weight, key_weight, value_weight, out_weight, band_reach, long_peers, long_count, send_tile):
    head_dim = D // HEADS
    score_scale = head_dim ** (-0.5)
    widened = features.astype(jnp.float32)
    normed = (widened * lax.rsqrt(lax.optimization_barrier(jnp.mean(widened * widened, axis=1, keepdims=True)) + EPSILON)).astype(jnp.bfloat16)
    queries = jnp.dot(normed, query_weight, preferred_element_type=jnp.float32).astype(jnp.bfloat16)
    keys_all = jnp.dot(normed, key_weight, preferred_element_type=jnp.float32).astype(jnp.bfloat16)
    values_all = jnp.dot(normed, value_weight, preferred_element_type=jnp.float32).astype(jnp.bfloat16)
    offsets = jnp.arange(3 * TILE, dtype=jnp.int32) - TILE
    places = jnp.arange(TILE, dtype=jnp.int32)
    inside_gap = jnp.abs(places[:, None] - offsets[None, :])
    portal_span = jnp.arange(PORTAL, dtype=jnp.int32)
    slot_ids = jnp.arange(MAXLONG, dtype=jnp.int32)

    def one_tile(tile_num):
        row_start = tile_num * TILE
        device_num = row_start // TOK_DEV
        group_num = device_num // N_RNG
        rank_num = device_num % N_RNG
        position = row_start - group_num * REGION
        band_rows = group_num * REGION + (position + offsets) % REGION
        sources = long_peers[tile_num] * N_RNG + rank_num
        portal_num = send_tile[sources, group_num]
        long_rows = (sources * TOK_DEV + portal_num * PORTAL)[:, None] + portal_span[None, :]
        key_rows = jnp.concatenate([band_rows.astype(jnp.int32), long_rows.reshape(-1).astype(jnp.int32)])
        query_blk = lax.dynamic_slice_in_dim(queries, row_start.astype(jnp.int32), TILE, 0)
        query_blk = query_blk.astype(jnp.float32).reshape(TILE, HEADS, head_dim)
        key_blk = jnp.take(keys_all, key_rows, axis=0).astype(jnp.float32).reshape(-1, HEADS, head_dim)
        value_blk = jnp.take(values_all, key_rows, axis=0).astype(jnp.float32).reshape(-1, HEADS, head_dim)
        scores = jnp.einsum('qhd,khd->hqk', query_blk, key_blk) * score_scale
        band_ok = inside_gap <= band_reach[device_num]
        long_ok = jnp.repeat(slot_ids < long_count[tile_num], PORTAL)
        allowed = jnp.concatenate([band_ok, jnp.broadcast_to(long_ok[None, :], (TILE, MAXLONG * PORTAL))], axis=1)
        scores = jnp.where(allowed[None], scores, -jnp.inf)
        highest = lax.optimization_barrier(jnp.max(scores, axis=2, keepdims=True))
        weights = jnp.exp(scores - highest)
        probabilities = (weights / lax.optimization_barrier(jnp.sum(weights, axis=2, keepdims=True))).astype(jnp.bfloat16)
        mixed = jnp.einsum('hqk,khd->qhd', probabilities.astype(jnp.float32), value_blk)
        return mixed.reshape(TILE, D).astype(jnp.bfloat16)
    attended = lax.map(one_tile, jnp.arange(QTILES, dtype=jnp.int32)).reshape(NODES, D)
    projected = jnp.dot(attended, out_weight, preferred_element_type=jnp.float32)
    return (widened + projected).astype(jnp.bfloat16)
```

```python
import functools

import jax
import jax.numpy as jnp
from jax import lax
from jax.experimental import pallas as pl
from jax.experimental.pallas import tpu as pltpu
from jax.sharding import PartitionSpec as P

HEADS = 16
TILE = 128
PORTAL = 64
MAXLONG = 6
EPSILON = 1e-06
LANES = 128
HEAD = 64
MIB = 1024 * 1024
SCALE2 = HEAD**-0.5 * 1.4426950408889634

VMEM = pl.BlockSpec(memory_space=pltpu.VMEM)
SMEM = pl.BlockSpec(memory_space=pltpu.SMEM)
ANY = pl.BlockSpec(memory_space=pl.ANY)


def pack_kernel(send_ref, feat_ref, normed_ref, out_ref, sems):
    widened = feat_ref[...].astype(jnp.float32)
    factor = lax.rsqrt(jnp.mean(widened * widened, axis=1, keepdims=True) + EPSILON)
    normed_ref[...] = (widened * factor).astype(jnp.bfloat16)
    copies = []
    for g in range(out_ref.shape[0]):
        start = pl.multiple_of(send_ref[0, g] * PORTAL, PORTAL)
        copies.append(
            pltpu.make_async_copy(
                normed_ref.at[pl.ds(start, PORTAL)], out_ref.at[g], sems.at[g]
            )
        )
    for copy in copies:
        copy.start()
    for copy in copies:
        copy.wait()


def project(x_ref, w_ref, out_ref, step=256):
    def body(i, carry):
        cols = pl.ds(pl.multiple_of(i * step, step), step)
        out_ref[:, cols] = jnp.dot(
            x_ref[...], w_ref[:, cols], preferred_element_type=jnp.float32
        ).astype(jnp.bfloat16)
        return carry

    lax.fori_loop(0, w_ref.shape[1] // step, body, 0)


def low_lanes():
    return lax.broadcasted_iota(jnp.int32, (TILE, LANES), 1) < HEAD


def pair_queries(q):
    low = low_lanes()
    zero = jnp.zeros_like(q)
    return jnp.concatenate([jnp.where(low, q, zero), jnp.where(low, zero, q)], axis=0)


def unpair(x):
    x = jnp.broadcast_to(x, (2 * TILE, LANES))
    return jnp.where(low_lanes(), x[:TILE], x[TILE:])


def pair_scores(q, k):
    return lax.dot_general(
        pair_queries(q), k, (((1,), (1,)), ((), ())), preferred_element_type=jnp.float32
    )


def band_kernel(
    reach_ref, normed_ref, lo_ref, hi_ref, wq_ref, wk_ref, wv_ref,
    q_ref, acc_ref, max_ref, sum_ref, x_s, k_s, v_s, bias_s,
):
    rows = normed_ref.shape[0]
    x_s[:TILE] = lo_ref[...]
    x_s[TILE : TILE + rows] = normed_ref[...]
    x_s[TILE + rows :] = hi_ref[...]
    place = lax.broadcasted_iota(jnp.int32, (2 * TILE, 3 * TILE), 0) % TILE
    key = lax.broadcasted_iota(jnp.int32, (2 * TILE, 3 * TILE), 1)
    inside = jnp.abs(place + TILE - key) <= reach_ref[0]
    bias_s[...] = jnp.where(inside, 0.0, -jnp.inf)
    project(normed_ref, wq_ref, q_ref)
    project(x_s, wk_ref, k_s)
    project(x_s, wv_ref, v_s)

    def body(h, carry):
        cols = pl.ds(pl.multiple_of(h * LANES, LANES), LANES)
        for t in range(rows // TILE):
            here = slice(t * TILE, (t + 1) * TILE)
            keys = slice(t * TILE, (t + 3) * TILE)
            s = pair_scores(q_ref[here, cols], k_s[keys, cols]) * SCALE2 + bias_s[...]
            m = jnp.max(s, axis=1, keepdims=True)
            p = jnp.exp2(s - m)
            acc = jnp.dot(
                p.astype(jnp.bfloat16), v_s[keys, cols], preferred_element_type=jnp.float32
            )
            max_ref[here, cols] = unpair(m)
            sum_ref[here, cols] = unpair(jnp.sum(p, axis=1, keepdims=True))
            acc_ref[here, cols] = unpair(acc)
        return carry

    lax.fori_loop(0, q_ref.shape[1] // LANES, body, 0)


def long_kernel(
    peers_ref, count_ref, arrived_ref, q_ref, acc_ref, max_ref, sum_ref, feat_ref,
    wk_ref, wv_ref, wo_ref, out_ref, x_s, k_s, v_s, att_s, sems,
):
    rows = q_ref.shape[0]
    span = MAXLONG * PORTAL
    copies = []
    for t in range(rows // TILE):
        for s in range(MAXLONG):
            copies.append(
                pltpu.make_async_copy(
                    arrived_ref.at[peers_ref[t, s]],
                    x_s.at[pl.ds((t * MAXLONG + s) * PORTAL, PORTAL)],
                    sems.at[t * MAXLONG + s],
                )
            )
    for copy in copies:
        copy.start()
    for copy in copies:
        copy.wait()
    project(x_s, wk_ref, k_s)
    project(x_s, wv_ref, v_s)
    slot = lax.broadcasted_iota(jnp.int32, (1, span), 1) // PORTAL

    def body(h, carry):
        cols = pl.ds(pl.multiple_of(h * LANES, LANES), LANES)
        for t in range(rows // TILE):
            here = slice(t * TILE, (t + 1) * TILE)
            keys = slice(t * span, (t + 1) * span)
            bias = jnp.where(slot < count_ref[t], 0.0, -jnp.inf)
            s = pair_scores(q_ref[here, cols], k_s[keys, cols]) * SCALE2 + bias
            band_max = max_ref[here, cols]
            band_max = jnp.concatenate(
                [band_max[:, :1], band_max[:, HEAD : HEAD + 1]], axis=0
            )
            m = jnp.maximum(jnp.max(s, axis=1, keepdims=True), band_max)
            p = jnp.exp2(s - m)
            acc = unpair(
                jnp.dot(
                    p.astype(jnp.bfloat16), v_s[keys, cols],
                    preferred_element_type=jnp.float32,
                )
            )
            total = unpair(jnp.sum(p, axis=1, keepdims=True))
            keep = unpair(jnp.exp2(band_max - m))
            acc = acc + keep * acc_ref[here, cols]
            total = total + keep * sum_ref[here, cols]
            att_s[here, cols] = (acc / total).astype(jnp.bfloat16)
        return carry

    lax.fori_loop(0, q_ref.shape[1] // LANES, body, 0)

    def out_body(i, carry):
        cols = pl.ds(pl.multiple_of(i * 256, 256), 256)
        projected = jnp.dot(att_s[...], wo_ref[:, cols], preferred_element_type=jnp.float32)
        out_ref[:, cols] = (feat_ref[:, cols].astype(jnp.float32) + projected).astype(
            jnp.bfloat16
        )
        return carry

    lax.fori_loop(0, wo_ref.shape[1] // 256, out_body, 0)


def shape(*dims, dtype=jnp.bfloat16):
    return jax.ShapeDtypeStruct(dims, dtype)


def local(
    features, query_weight, key_weight, value_weight, out_weight,
    band_reach, long_peers, long_count, send_tile,
):
    rows, width = features.shape
    groups = lax.axis_size("grp")
    ranks = lax.axis_size("rng")
    normed, outgoing = pl.pallas_call(
        pack_kernel,
        out_shape=(shape(rows, width), shape(groups, PORTAL, width)),
        in_specs=[SMEM, VMEM],
        out_specs=(VMEM, ANY),
        scratch_shapes=[pltpu.SemaphoreType.DMA((groups,))],
        compiler_params=pltpu.CompilerParams(vmem_limit_bytes=8 * MIB),
        name="pack",
    )(send_tile, features)
    arrived = lax.all_to_all(outgoing, "grp", split_axis=0, concat_axis=0, tiled=True)
    up = [(i, (i + 1) % ranks) for i in range(ranks)]
    down = [(i, (i - 1) % ranks) for i in range(ranks)]
    lo = lax.ppermute(normed[rows - TILE :], "rng", up)
    hi = lax.ppermute(normed[:TILE], "rng", down)
    wide = shape(rows, width, dtype=jnp.float32)
    ext = rows + 2 * TILE
    queries, acc, top, total = pl.pallas_call(
        band_kernel,
        out_shape=(shape(rows, width), wide, wide, wide),
        in_specs=[SMEM] + [VMEM] * 6,
        out_specs=(VMEM,) * 4,
        scratch_shapes=[pltpu.VMEM((ext, width), jnp.bfloat16)] * 3
        + [pltpu.VMEM((2 * TILE, 3 * TILE), jnp.float32)],
        compiler_params=pltpu.CompilerParams(vmem_limit_bytes=24 * MIB),
        name="band",
    )(band_reach, normed, lo, hi, query_weight, key_weight, value_weight)
    tiles = rows // TILE
    keys = tiles * MAXLONG * PORTAL
    return pl.pallas_call(
        long_kernel,
        out_shape=shape(rows, width),
        in_specs=[SMEM, SMEM, ANY] + [VMEM] * 8,
        out_specs=VMEM,
        scratch_shapes=[pltpu.VMEM((keys, width), jnp.bfloat16)] * 3
        + [pltpu.VMEM((rows, width), jnp.bfloat16), pltpu.SemaphoreType.DMA((tiles * MAXLONG,))],
        compiler_params=pltpu.CompilerParams(vmem_limit_bytes=24 * MIB),
        name="long",
    )(
        long_peers, long_count, arrived, queries, acc, top, total, features,
        key_weight, value_weight, out_weight,
    )


def solution(mesh):
    spread = ("grp", "rng")
    return jax.shard_map(
        local,
        mesh=mesh,
        in_specs=(
            P(spread, None), P(), P(), P(), P(),
            P(spread), P(spread, None), P(spread), P(spread, None),
        ),
        out_specs=P(spread, None),
        check_vma=False,
    )
```

```python
import jax
import jax.numpy as jnp
from jax import lax
from jax.experimental import pallas as pl
from jax.experimental.pallas import tpu as pltpu
from jax.sharding import PartitionSpec as P


TILE = 128
PORTAL = 64
MAXLONG = 6
EPSILON = 1e-06
LANES = 128
HEAD = 64
BLOCK = 256
PICKS = 8
EARLY = 9
LATE = 6
MIB = 1024 * 1024
SCALE2 = HEAD**-0.5 * 1.4426950408889634
F32 = jnp.float32
BF16 = jnp.bfloat16

VMEM = pl.BlockSpec(memory_space=pltpu.VMEM)
SMEM = pl.BlockSpec(memory_space=pltpu.SMEM)


def region(x, y, c):
    return (x % 4) * 4 + (y % 2) * 2 + c % 2


def moved(dx, dy, dc):
    return [
        (region(x, y, c), region(x + dx, y + dy, c ^ dc))
        for x in range(4)
        for y in range(2)
        for c in range(2)
    ]


def place_of(index):
    return index // 4, (index // 2) % 2, index % 2


def pack_kernel(send_ref, feat_ref, a_ref, x1_ref, x2_ref, x3_ref, up_ref, down_ref, mate_ref):
    rows = feat_ref.shape[0]
    widened = feat_ref[...].astype(F32)
    factor = lax.rsqrt(jnp.mean(widened * widened, axis=1, keepdims=True) + EPSILON)
    normed = (widened * factor).astype(BF16)
    a_ref[:rows] = normed
    down_ref[...] = normed[:TILE]
    up_ref[...] = normed[rows - TILE :]
    x, y, c = place_of(lax.axis_index("grp"))

    def tile(dx, dy, dc):
        pick = send_ref[0, ((x + dx) % 4) * 4 + (y ^ dy) * 2 + (c ^ dc)]
        return pick

    def rows_of(pick):
        return a_ref[pl.ds(pl.multiple_of(pick * PORTAL, PORTAL), PORTAL)]

    for dx, ref in ((1, x1_ref), (2, x2_ref), (3, x3_ref)):
        for dc in range(2):
            ref[dc * PORTAL : (dc + 1) * PORTAL] = rows_of(tile(dx, 0, dc))
    mate_ref[...] = rows_of(tile(0, 0, 1))
    row = lax.broadcasted_iota(jnp.int32, (PICKS, feat_ref.shape[1]), 0)
    picks = jnp.zeros(row.shape, jnp.int32)
    for i in range(PICKS):
        picks = jnp.where(row == i, tile(i // 2, 1, i % 2), picks)
    a_ref[rows:] = picks.astype(F32).astype(BF16)


def relay_kernel(a_ref, *out_refs):
    rows = a_ref.shape[0] - PICKS
    picks = a_ref[rows:].astype(F32)
    for i, ref in enumerate(out_refs):
        pick = jnp.broadcast_to(picks[i : i + 1], (PORTAL, picks.shape[1]))
        tile = a_ref[:PORTAL].astype(F32)
        for k in range(1, rows // PORTAL):
            tile = jnp.where(
                pick == float(k), a_ref[k * PORTAL : (k + 1) * PORTAL].astype(F32), tile
            )
        ref[...] = tile.astype(BF16)


def dot(x, w):
    return jnp.dot(x, w, preferred_element_type=F32)


def local_kernel(a_ref, wq_ref, wk_ref, wv_ref, q_ref, k_ref, v_ref):
    rows = q_ref.shape[0]
    normed = a_ref[:rows]
    q_ref[...] = dot(normed, wq_ref[...]).astype(BF16)
    k_ref[...] = dot(normed, wk_ref[...]).astype(BF16)
    v_ref[...] = dot(normed, wv_ref[...]).astype(BF16)


def low_lanes():
    return lax.broadcasted_iota(jnp.int32, (TILE, LANES), 1) < HEAD


def pair_queries(q):
    low = low_lanes()
    zero = jnp.zeros_like(q)
    return jnp.concatenate([jnp.where(low, q, zero), jnp.where(low, zero, q)], axis=0)


def unpair(x):
    x = jnp.broadcast_to(x, (2 * TILE, LANES))
    return jnp.where(low_lanes(), x[:TILE], x[TILE:])


def pair_scores(q, k):
    return lax.dot_general(
        pair_queries(q), k, (((1,), (1,)), ((), ())), preferred_element_type=F32
    )


def band_kernel(
    reach_ref, q_ref, k_ref, v_ref, lo_ref, hi_ref, wk_ref, wv_ref,
    acc_ref, max_ref, sum_ref, x_s, k_s, v_s, bias_s,
):
    rows = q_ref.shape[0]

    @pl.when(pl.program_id(0) == 0)
    def _():
        x_s[:TILE] = lo_ref[...]
        x_s[TILE:] = hi_ref[...]
        place = lax.broadcasted_iota(jnp.int32, bias_s.shape, 0) % TILE
        key = lax.broadcasted_iota(jnp.int32, bias_s.shape, 1)
        inside = jnp.abs(place + TILE - key) <= reach_ref[0]
        bias_s[...] = jnp.where(inside, 0.0, -jnp.inf)

    for w_ref, here_ref, ext in ((wk_ref, k_ref, k_s), (wv_ref, v_ref, v_s)):
        rim = dot(x_s[...], w_ref[...]).astype(BF16)
        ext[:TILE] = rim[:TILE]
        ext[TILE : TILE + rows] = here_ref[...]
        ext[TILE + rows :] = rim[TILE:]
    for h in range(q_ref.shape[1] // LANES):
        cols = slice(h * LANES, (h + 1) * LANES)
        for t in range(rows // TILE):
            here = slice(t * TILE, (t + 1) * TILE)
            keys = slice(t * TILE, (t + 3) * TILE)
            s = pair_scores(q_ref[here, cols], k_s[keys, cols]) * SCALE2 + bias_s[...]
            m = jnp.max(s, axis=1, keepdims=True)
            p = jnp.exp2(s - m)
            acc = dot(p.astype(BF16), v_s[keys, cols])
            max_ref[here, cols] = unpair(m)
            sum_ref[here, cols] = unpair(jnp.sum(p, axis=1, keepdims=True))
            acc_ref[here, cols] = unpair(acc)


def early_kernel(*refs):
    (_, mine_ref, x1_ref, x2_ref, x3_ref, swap_ref, wk_ref, wv_ref, k_ref, v_ref, x_s) = refs

    @pl.when(pl.program_id(0) == 0)
    def _():
        def put(pos, ref, start):
            x_s[(pos - 1) * PORTAL : pos * PORTAL] = ref[start * PORTAL : (start + 1) * PORTAL]

        put(8, mine_ref, 0)
        for dx, ref in ((1, x1_ref), (2, x2_ref), (3, x3_ref)):
            put(2 * dx, ref, 0)
        for i, pos in enumerate((1, 9, 3, 5, 7)):
            put(pos, swap_ref, i)

    k_ref[...] = dot(x_s[...], wk_ref[...]).astype(BF16)
    v_ref[...] = dot(x_s[...], wv_ref[...]).astype(BF16)


def late_kernel(
    peers_ref, count_ref, q_ref, acc_ref, max_ref, sum_ref, feat_ref, ke_ref, ve_ref,
    l0, l1, l2, l3, l4, l5, wk_ref, wv_ref, wo_ref, out_ref, x_s, k_s, v_s, out_s,
):
    rows = q_ref.shape[0]
    span = MAXLONG * PORTAL
    step = pl.program_id(0)

    @pl.when(step == 0)
    def _():
        for i, ref in enumerate((l0, l1, l2, l3, l4, l5)):
            x_s[i * PORTAL : (i + 1) * PORTAL] = ref[...]

    split = EARLY * PORTAL
    k_s[:split] = ke_ref[...]
    v_s[:split] = ve_ref[...]
    k_s[split:] = dot(x_s[...], wk_ref[...]).astype(BF16)
    v_s[split:] = dot(x_s[...], wv_ref[...]).astype(BF16)
    x, y, c = place_of(lax.axis_index("grp"))
    slot = lax.broadcasted_iota(jnp.int32, (1, span), 1) // PORTAL
    attended = []
    for h in range(q_ref.shape[1] // LANES):
        cols = slice(h * LANES, (h + 1) * LANES)
        tiles = []
        for t in range(rows // TILE):
            here = slice(t * TILE, (t + 1) * TILE)
            starts = []
            for s in range(MAXLONG):
                px, py, pc = place_of(peers_ref[t, s])
                pos = (y ^ py) * 8 + ((x - px + 4) % 4) * 2 + (c ^ pc)
                starts.append(pl.multiple_of((pos - 1) * PORTAL, PORTAL))
            keys = jnp.concatenate([k_s[pl.ds(i, PORTAL), cols] for i in starts], axis=0)
            values = jnp.concatenate([v_s[pl.ds(i, PORTAL), cols] for i in starts], axis=0)
            bias = jnp.where(slot < count_ref[t], 0.0, -jnp.inf)
            s = pair_scores(q_ref[here, cols], keys) * SCALE2 + bias
            band_max = max_ref[here, cols]
            band_max = jnp.concatenate(
                [band_max[:, :1], band_max[:, HEAD : HEAD + 1]], axis=0
            )
            m = jnp.maximum(jnp.max(s, axis=1, keepdims=True), band_max)
            p = jnp.exp2(s - m)
            acc = unpair(dot(p.astype(BF16), values))
            total = unpair(jnp.sum(p, axis=1, keepdims=True))
            keep = unpair(jnp.exp2(band_max - m))
            acc = acc + keep * acc_ref[here, cols]
            total = total + keep * sum_ref[here, cols]
            tiles.append((acc / total).astype(BF16))
        attended.append(jnp.concatenate(tiles, axis=0))
    part = dot(jnp.concatenate(attended, axis=1), wo_ref[...])

    @pl.when(step == 0)
    def _():
        out_s[...] = feat_ref[...].astype(F32) + part

    @pl.when(step > 0)
    def _():
        out_s[...] = out_s[...] + part

    @pl.when(step == pl.num_programs(0) - 1)
    def _():
        out_ref[...] = out_s[...].astype(BF16)


def named(kernel, **kw):
    def run(*args):
        return pl.pallas_call(kernel, **kw)(*args)

    return run


def shape(*dims, dtype=BF16):
    return jax.ShapeDtypeStruct(dims, dtype)


def cols_of(rows, block=BLOCK):
    return pl.BlockSpec((rows, block), lambda i: (0, i))


def whole(rows, width):
    return pl.BlockSpec((rows, width), lambda i: (0, 0))


def params(mib):
    return pltpu.CompilerParams(vmem_limit_bytes=mib * MIB)


def local(
    features, query_weight, key_weight, value_weight, out_weight,
    band_reach, long_peers, long_count, send_tile,
):
    rows, width = features.shape
    ranks = lax.axis_size("rng")
    steps = width // BLOCK
    tall = shape(2 * PORTAL, width)
    half = shape(TILE, width)
    tile = shape(PORTAL, width)
    a, x1, x2, x3, up, down, mate = named(pack_kernel,
        out_shape=(shape(rows + PICKS, width), tall, tall, tall, half, half, tile),
        in_specs=[SMEM, VMEM],
        out_specs=(VMEM,) * 7,
        compiler_params=params(8),
    )(send_tile, features)
    across = lax.ppermute(a, "grp", moved(0, 1, 0))
    x1, x2, x3 = [
        lax.ppermute(part, "grp", moved(dx, 0, 0))
        for dx, part in ((1, x1), (2, x2), (3, x3))
    ]
    lo = lax.ppermute(up, "rng", [(i, (i + 1) % ranks) for i in range(ranks)])
    hi = lax.ppermute(down, "rng", [(i, (i - 1) % ranks) for i in range(ranks)])
    square = shape(rows, width)
    w_cols = cols_of(width)
    queries, keys, values = named(local_kernel,
        grid=(steps,),
        out_shape=(square,) * 3,
        in_specs=[whole(rows + PICKS, width)] + [w_cols] * 3,
        out_specs=(cols_of(rows),) * 3,
        compiler_params=params(16),
    )(a, query_weight, key_weight, value_weight)
    relayed = named(relay_kernel,
        out_shape=(tile,) * PICKS,
        in_specs=[VMEM],
        out_specs=(VMEM,) * PICKS,
        compiler_params=params(8),
    )(across)
    late = [lax.ppermute(relayed[i], "grp", moved(i // 2, 0, i % 2)) for i in range(2, PICKS)]
    swapped = lax.ppermute(
        jnp.concatenate([mate, relayed[1], x1[PORTAL:], x2[PORTAL:], x3[PORTAL:]], axis=0),
        "grp",
        moved(0, 0, 1),
    )
    wide = shape(rows, width, dtype=F32)
    acc, top, total = named(band_kernel,
        grid=(steps,),
        out_shape=(wide,) * 3,
        in_specs=[SMEM] + [cols_of(rows)] * 3 + [whole(TILE, width)] * 2 + [w_cols] * 2,
        out_specs=(cols_of(rows),) * 3,
        scratch_shapes=[
            pltpu.VMEM((2 * TILE, width), BF16),
            pltpu.VMEM((rows + 2 * TILE, BLOCK), BF16),
            pltpu.VMEM((rows + 2 * TILE, BLOCK), BF16),
            pltpu.VMEM((2 * TILE, 3 * TILE), F32),
        ],
        compiler_params=params(16),
    )(band_reach, queries, keys, values, lo, hi, key_weight, value_weight)
    early_rows = EARLY * PORTAL
    early_keys, early_values = named(early_kernel,
        grid=(steps,),
        out_shape=(shape(early_rows, width),) * 2,
        in_specs=[whole(PORTAL, width)] * 2
        + [whole(2 * PORTAL, width)] * 3
        + [whole(5 * PORTAL, width)]
        + [w_cols] * 2,
        out_specs=(cols_of(early_rows),) * 2,
        scratch_shapes=[pltpu.VMEM((early_rows, width), BF16)],
        compiler_params=params(16),
    )(mate, relayed[0], x1, x2, x3, swapped, key_weight, value_weight)
    late_rows = LATE * PORTAL
    return named(late_kernel,
        grid=(steps,),
        out_shape=square,
        in_specs=[SMEM, SMEM]
        + [cols_of(rows)] * 4
        + [whole(rows, width)]
        + [cols_of(early_rows)] * 2
        + [whole(PORTAL, width)] * LATE
        + [w_cols] * 2
        + [pl.BlockSpec((BLOCK, width), lambda i: (i, 0))],
        out_specs=whole(rows, width),
        scratch_shapes=[
            pltpu.VMEM((late_rows, width), BF16),
            pltpu.VMEM((early_rows + late_rows, BLOCK), BF16),
            pltpu.VMEM((early_rows + late_rows, BLOCK), BF16),
            pltpu.VMEM((rows, width), F32),
        ],
        compiler_params=params(20),
    )(
        long_peers, long_count, queries, acc, top, total, features, early_keys, early_values,
        *late, key_weight, value_weight, out_weight,
    )


def solution(mesh):
    spread = ("grp", "rng")
    return jax.shard_map(
        local,
        mesh=mesh,
        in_specs=(
            P(spread, None), P(), P(), P(), P(),
            P(spread), P(spread, None), P(spread), P(spread, None),
        ),
        out_specs=P(spread, None),
        check_vma=False,
    )
```

```python
import jax
import jax.numpy as jnp
from jax import lax
from jax.experimental import pallas as pl
from jax.experimental.pallas import tpu as pltpu
from jax.sharding import PartitionSpec as P


TILE = 128
PORTAL = 64
MAXLONG = 6
EPSILON = 1e-06
LANES = 128
HEAD = 64
CHUNK = 64
BLOCK = 256
PICKS = 8
SLOTS = 15
RIM = SLOTS * PORTAL
FIRST = (1, 2, 3, 4, 5, 6, 7, 8, 9, 12, 13)
SECOND = (10, 11, 14, 15)
MIB = 1024 * 1024
SCALE2 = HEAD**-0.5 * 1.4426950408889634
F32 = jnp.float32
NEVER = float(jnp.finfo(jnp.bfloat16).min)
BF16 = jnp.bfloat16

VMEM = pl.BlockSpec(memory_space=pltpu.VMEM)
SMEM = pl.BlockSpec(memory_space=pltpu.SMEM)
HBM = pl.BlockSpec(memory_space=pltpu.HBM)


def region(x, y, c):
    return (x % 4) * 4 + (y % 2) * 2 + c % 2


def moved(dx, dy, dc):
    return [
        (region(x, y, c), region(x + dx, y + dy, c ^ dc))
        for x in range(4)
        for y in range(2)
        for c in range(2)
    ]


def place_of(index):
    return index // 4, (index // 2) % 2, index % 2


def norm_kernel(feat_ref, a_ref, up_ref, down_ref):
    rows = feat_ref.shape[0]
    widened = feat_ref[...].astype(F32)
    factor = lax.rsqrt(jnp.mean(widened * widened, axis=1, keepdims=True) + EPSILON)
    normed = (widened * factor).astype(BF16)
    a_ref[...] = normed
    down_ref[...] = normed[:TILE]
    up_ref[...] = normed[rows - TILE :]


def pack_kernel(send_ref, a_ref, x1_ref, x2_ref, x3_ref, mate_ref, picks_ref):
    x, y, c = place_of(lax.axis_index("grp"))

    def pick(dx, dy, dc):
        return send_ref[0, ((x + dx) % 4) * 4 + (y ^ dy) * 2 + (c ^ dc)]

    def tile(index):
        return a_ref[pl.ds(pl.multiple_of(index * PORTAL, PORTAL), PORTAL)]

    for dx, ref in ((1, x1_ref), (2, x2_ref), (3, x3_ref)):
        for dc in range(2):
            ref[dc * PORTAL : (dc + 1) * PORTAL] = tile(pick(dx, 0, dc))
    mate_ref[...] = tile(pick(0, 0, 1))
    row = lax.broadcasted_iota(jnp.int32, picks_ref.shape, 0)
    picks = jnp.zeros(row.shape, jnp.int32)
    for i in range(PICKS):
        picks = jnp.where(row == i, pick(i // 2, 1, i % 2), picks)
    picks_ref[...] = picks.astype(F32).astype(BF16)


def relay_kernel(a_ref, picks_ref, *out_refs):
    rows = a_ref.shape[0]
    picks = picks_ref[...].astype(F32)
    for i, ref in enumerate(out_refs):
        pick = jnp.broadcast_to(picks[i : i + 1], (PORTAL, picks.shape[1]))
        tile = a_ref[:PORTAL].astype(F32)
        for k in range(1, rows // PORTAL):
            tile = jnp.where(
                pick == float(k), a_ref[k * PORTAL : (k + 1) * PORTAL].astype(F32), tile
            )
        ref[...] = tile.astype(BF16)


def dot(x, w):
    return jnp.dot(x, w, preferred_element_type=F32)


def block_cols(b):
    return slice(b * BLOCK, (b + 1) * BLOCK)


def low_lanes():
    return lax.broadcasted_iota(jnp.int32, (TILE, LANES), 1) < HEAD


def pair_queries(q):
    low = low_lanes()
    zero = jnp.zeros_like(q)
    return jnp.concatenate([jnp.where(low, q, zero), jnp.where(low, zero, q)], axis=0)


def unpair(x):
    return jnp.where(low_lanes(), x[:TILE], x[TILE:])


def set_eye(eye_ref):
    row = lax.broadcasted_iota(jnp.int32, eye_ref.shape, 0) % TILE
    lane = lax.broadcasted_iota(jnp.int32, eye_ref.shape, 1)
    eye_ref[...] = jnp.where(row == lane, 1.0, 0.0).astype(BF16)


def masked(keep):
    return jnp.where(keep, 0.0, NEVER).astype(BF16)


def pair_scores(q, eye, keys, mask):
    return lax.dot_general(
        jnp.concatenate([pair_queries(q), eye], axis=1),
        jnp.concatenate([keys, mask], axis=1),
        (((1,), (1,)), ((), ())),
        preferred_element_type=F32,
    )


def weigh(p, values):
    ones = jnp.ones(values.shape, BF16)
    both = dot(p, jnp.concatenate([values, ones], axis=1))
    return unpair(both[:, :LANES]), unpair(both[:, LANES:])


def chain(j, tiles):
    h, t = j // tiles, j % tiles
    return t, slice(t * TILE, (t + 1) * TILE), slice(h * LANES, (h + 1) * LANES)


def staged(count, fill, first, second, third):
    for j in range(count + 2):
        fill(j)
        if j < count:
            first(j)
        if 0 <= j - 1 < count:
            second(j - 1)
        if 0 <= j - 2:
            third(j - 2)


def spread_fill(parts, per_block):
    def fill(j):
        if j == 0:
            for part in parts:
                part(0)
        b, i = j // per_block + 1, j % per_block
        if i < len(parts):
            parts[i](b)

    return fill


def here_kernel(
    reach_ref, a_ref, wq_ref, wk_ref, wv_ref, q_ref, acc_ref, max_ref, sum_ref,
    k_s, v_s, eye_s, mask_s, s0, s1, p0, p1,
):
    rows, width = q_ref.shape
    tiles = rows // TILE
    blocks = width // BLOCK
    s_s, p_s = (s0, s1), (p0, p1)
    set_eye(eye_s)
    key = lax.broadcasted_iota(jnp.int32, (rows, LANES), 0)
    place = lax.broadcasted_iota(jnp.int32, (rows, LANES), 1)
    for t in range(tiles):
        mask_s[t * rows : (t + 1) * rows] = masked(jnp.abs(place + t * TILE - key) <= reach_ref[0])

    def project(w_ref, out_ref, scale=None):
        def part(b):
            if b < blocks:
                cols = block_cols(b)
                product = dot(a_ref[:rows], w_ref[:, cols])
                if scale is not None:
                    product = product * scale
                out_ref[:, cols] = product.astype(BF16)

        return part

    def first(j):
        t, here, cols = chain(j, tiles)
        mask = mask_s[t * rows : (t + 1) * rows]
        s_s[j % 2][...] = pair_scores(q_ref[here, cols], eye_s[...], k_s[:, cols], mask)

    def second(j):
        for r in range(0, 2 * TILE, CHUNK):
            s = s_s[j % 2][r : r + CHUNK]
            m = jnp.max(s, axis=1, keepdims=True)
            max_ref[j, r : r + CHUNK] = jnp.broadcast_to(m, (CHUNK, LANES))
            p_s[j % 2][r : r + CHUNK] = jnp.exp2(s - m).astype(BF16)

    def third(j):
        _, here, cols = chain(j, tiles)
        acc, total = weigh(p_s[j % 2][...], v_s[:, cols])
        acc_ref[here, cols] = acc
        sum_ref[here, cols] = total

    fill = spread_fill(
        [project(wq_ref, q_ref, SCALE2), project(wk_ref, k_s), project(wv_ref, v_s)],
        tiles * BLOCK // LANES,
    )
    staged(tiles * width // LANES, fill, first, second, third)


def tile_rows(pos):
    return slice((pos - 1) * PORTAL, pos * PORTAL)


def far_kernel(
    mine_ref, l1_ref, l4_ref, l5_ref, x1_ref, x2_ref, x3_ref, swap_ref, lo_ref, hi_ref,
    wk_ref, wv_ref, ke_ref, ve_ref, x_s,
):
    tiles = {8: mine_ref[...], 9: l1_ref[...], 12: l4_ref[...], 13: l5_ref[...]}
    for dx, ref in ((1, x1_ref), (2, x2_ref), (3, x3_ref)):
        tiles[2 * dx] = ref[:PORTAL]
    for i, pos in enumerate((1, 3, 5, 7)):
        tiles[pos] = swap_ref[i * PORTAL : (i + 1) * PORTAL]
    for i, pos in enumerate(FIRST):
        x_s[tile_rows(i + 1)] = tiles[pos]
    near = len(FIRST) * PORTAL
    x_s[near : near + TILE] = lo_ref[...]
    x_s[near + TILE :] = hi_ref[...]
    for b in range(wk_ref.shape[1] // BLOCK):
        cols = block_cols(b)
        for w_ref, out_ref in ((wk_ref, ke_ref), (wv_ref, ve_ref)):
            product = dot(x_s[...], w_ref[:, cols]).astype(BF16)
            for i, pos in enumerate(FIRST):
                out_ref[tile_rows(pos), cols] = product[tile_rows(i + 1)]
            out_ref[RIM:, cols] = product[near:]


def last_kernel(
    peers_hbm, count_hbm, reach_ref, q_ref, acc_ref, max_ref, sum_ref, feat_ref, ke_ref, ve_ref,
    l0, l1, l2, l3, wk_ref, wv_ref, wo_ref, out_hbm, k_ref, v_ref,
    x_s, att_s, kl_s, vl_s, eye_s, mask_s, keep0, keep1, s0, s1, p0, p1, out_s,
    peers_ref, count_ref, sems,
):
    rows, width = q_ref.shape
    tiles = rows // TILE
    blocks = width // BLOCK
    span = MAXLONG * PORTAL
    keys = span + TILE
    s_s, p_s, keep_s = (s0, s1), (p0, p1), (keep0, keep1)
    peers_copy = pltpu.make_async_copy(peers_hbm, peers_ref, sems.at[0])
    count_copy = pltpu.make_async_copy(count_hbm, count_ref, sems.at[1])
    peers_copy.start()
    count_copy.start()
    for i, ref in enumerate((l0, l1, l2, l3)):
        x_s[i * PORTAL : (i + 1) * PORTAL] = ref[...]
    x, y, c = place_of(lax.axis_index("grp"))
    set_eye(eye_s)
    near = lax.broadcasted_iota(jnp.int32, (TILE, LANES), 0)
    place = lax.broadcasted_iota(jnp.int32, (TILE, LANES), 1)
    slot = lax.broadcasted_iota(jnp.int32, (span, LANES), 0) // PORTAL
    for t in range(tiles):
        gap = place + TILE - near if t == 0 else near + TILE - place
        mask_s[t * keys + span : (t + 1) * keys] = masked(gap <= reach_ref[0])
    starts = []

    def lists():
        peers_copy.wait()
        count_copy.wait()
        for t in range(tiles):
            mask_s[t * keys : t * keys + span] = masked(slot < count_ref[t])
            for s in range(MAXLONG):
                px, py, pc = place_of(peers_ref[t, s])
                pos = (y ^ py) * 8 + ((x - px + 4) % 4) * 2 + (c ^ pc)
                starts.append(pl.multiple_of((pos - 1) * PORTAL, PORTAL))

    def project(w_ref, all_ref, listed_ref):
        def part(b):
            if b < blocks:
                cols = block_cols(b)
                product = dot(x_s[...], w_ref[:, cols]).astype(BF16)
                for i, pos in enumerate(SECOND):
                    all_ref[tile_rows(pos), cols] = product[tile_rows(i + 1)]
                if not starts:
                    lists()
                for t in range(tiles):
                    for s in range(MAXLONG):
                        row = t * keys + s * PORTAL
                        listed_ref[row : row + PORTAL, cols] = all_ref[
                            pl.ds(starts[t * MAXLONG + s], PORTAL), cols
                        ]
                    rim = RIM + t * TILE
                    listed_ref[t * keys + span : (t + 1) * keys, cols] = all_ref[
                        rim : rim + TILE, cols
                    ]

        return part

    def first(j):
        t, here, cols = chain(j, tiles)
        mine = slice(t * keys, (t + 1) * keys)
        s_s[j % 2][...] = pair_scores(q_ref[here, cols], eye_s[...], kl_s[mine, cols], mask_s[mine])

    def second(j):
        for r in range(0, 2 * TILE, CHUNK):
            s = s_s[j % 2][r : r + CHUNK]
            band_max = max_ref[j, r : r + CHUNK]
            m = jnp.maximum(jnp.max(s, axis=1, keepdims=True), band_max)
            keep_s[j % 2][r : r + CHUNK] = jnp.exp2(band_max - m)
            p = jnp.exp2(s - jnp.concatenate([m] * (keys // LANES), axis=1))
            p_s[j % 2][r : r + CHUNK] = p.astype(BF16)

    def third(j):
        t, here, cols = chain(j, tiles)
        acc, total = weigh(p_s[j % 2][...], vl_s[t * keys : (t + 1) * keys, cols])
        keep = unpair(keep_s[j % 2][...])
        acc = acc + keep * acc_ref[here, cols]
        total = total + keep * sum_ref[here, cols]
        att_s[here, cols] = (acc / total).astype(BF16)

    fill = spread_fill(
        [project(wk_ref, k_ref, kl_s), project(wv_ref, v_ref, vl_s)], tiles * BLOCK // LANES
    )
    staged(tiles * width // LANES, fill, first, second, third)
    copies = []
    for b in range(blocks):
        cols = block_cols(b)
        projected = dot(att_s[...], wo_ref[:, cols])
        out_s[:, cols] = (feat_ref[:, cols].astype(F32) + projected).astype(BF16)
        copies.append(
            pltpu.make_async_copy(out_s.at[:, cols], out_hbm.at[:, cols], sems.at[2 + b])
        )
        copies[-1].start()
    for copy in copies:
        copy.wait()


def named(kernel, **kw):
    def run(*args):
        return pl.pallas_call(kernel, **kw)(*args)

    return run


def shape(*dims, dtype=BF16):
    return jax.ShapeDtypeStruct(dims, dtype)


def params(mib):
    return pltpu.CompilerParams(vmem_limit_bytes=mib * MIB)


def local(
    features, query_weight, key_weight, value_weight, out_weight,
    band_reach, long_peers, long_count, send_tile,
):
    rows, width = features.shape
    ranks = lax.axis_size("rng")
    tall = shape(2 * PORTAL, width)
    half = shape(TILE, width)
    tile = shape(PORTAL, width)
    square = shape(rows, width)
    a, up, down = named(
        norm_kernel,
        out_shape=(square, half, half),
        in_specs=[VMEM],
        out_specs=(VMEM,) * 3,
        compiler_params=params(4),
    )(features)
    across = lax.ppermute(a, "grp", moved(0, 1, 0))
    x1, x2, x3, mate, picks = named(
        pack_kernel,
        out_shape=(tall, tall, tall, tile, shape(PICKS, width)),
        in_specs=[SMEM, VMEM],
        out_specs=(VMEM,) * 5,
        cost_estimate=pl.CostEstimate(flops=10**10, bytes_accessed=2**23, transcendentals=0),
        compiler_params=params(4),
    )(send_tile, a)
    x1, x2, x3 = [
        lax.ppermute(part, "grp", moved(dx, 0, 0))
        for dx, part in ((1, x1), (2, x2), (3, x3))
    ]
    picks = lax.ppermute(picks, "grp", moved(0, 1, 0))
    wide = shape(rows, width, dtype=F32)
    chains = rows // TILE * width // LANES
    tops = shape(chains, 2 * TILE, LANES, dtype=F32)

    def stages(keys):
        return [pltpu.VMEM((2 * TILE, keys), F32)] * 2 + [pltpu.VMEM((2 * TILE, keys), BF16)] * 2

    queries, acc, top, total = named(
        here_kernel,
        out_shape=(square, wide, tops, wide),
        in_specs=[SMEM] + [VMEM] * 4,
        out_specs=(VMEM,) * 4,
        scratch_shapes=[pltpu.VMEM((rows, width), BF16)] * 2
        + [pltpu.VMEM((2 * TILE, LANES), BF16), pltpu.VMEM((rows // TILE * rows, LANES), BF16)]
        + stages(rows),
        compiler_params=params(8),
    )(band_reach, a, query_weight, key_weight, value_weight)
    up, down, queries, x1, x3 = lax.optimization_barrier((up, down, queries, x1, x3))
    lo = lax.ppermute(up, "rng", [(i, (i + 1) % ranks) for i in range(ranks)])
    hi = lax.ppermute(down, "rng", [(i, (i - 1) % ranks) for i in range(ranks)])
    relayed = named(
        relay_kernel,
        out_shape=(tile,) * PICKS,
        in_specs=[VMEM] * 2,
        out_specs=(VMEM,) * PICKS,
        compiler_params=params(4),
    )(across, picks)
    late = {i: lax.ppermute(relayed[i], "grp", moved(i // 2, 0, i % 2)) for i in range(1, PICKS)}
    swapped = lax.ppermute(
        jnp.concatenate([mate, x1[PORTAL:], x2[PORTAL:], x3[PORTAL:]], axis=0),
        "grp",
        moved(0, 0, 1),
    )
    far = shape(RIM + 2 * TILE, width)
    far_rows = len(FIRST) * PORTAL + 2 * TILE
    far_keys, far_values = named(
        far_kernel,
        out_shape=(far, far),
        in_specs=[VMEM] * 12,
        out_specs=(VMEM,) * 2,
        scratch_shapes=[pltpu.VMEM((far_rows, width), BF16)],
        compiler_params=params(8),
    )(
        relayed[0], late[1], late[4], late[5], x1, x2, x3, swapped, lo, hi,
        key_weight, value_weight,
    )
    span = MAXLONG * PORTAL + TILE
    listed = rows // TILE * span
    updated, _, _ = named(
        last_kernel,
        out_shape=(square, far, far),
        in_specs=[HBM, HBM, SMEM] + [VMEM] * (7 + len(SECOND) + 3),
        out_specs=(HBM, VMEM, VMEM),
        scratch_shapes=[
            pltpu.VMEM((len(SECOND) * PORTAL, width), BF16),
            pltpu.VMEM((rows, width), BF16),
            pltpu.VMEM((listed, width), BF16),
            pltpu.VMEM((listed, width), BF16),
            pltpu.VMEM((2 * TILE, LANES), BF16),
            pltpu.VMEM((listed, LANES), BF16),
            pltpu.VMEM((2 * TILE, LANES), F32),
            pltpu.VMEM((2 * TILE, LANES), F32),
        ]
        + stages(span)
        + [
            pltpu.VMEM((rows, width), BF16),
            pltpu.SMEM(long_peers.shape, jnp.int32),
            pltpu.SMEM(long_count.shape, jnp.int32),
            pltpu.SemaphoreType.DMA((2 + width // BLOCK,)),
        ],
        input_output_aliases={8: 1, 9: 2},
        compiler_params=params(14),
    )(
        long_peers, long_count, band_reach, queries, acc, top, total, features,
        far_keys, far_values, late[2], late[3], late[6], late[7], key_weight, value_weight, out_weight,
    )
    return updated


def solution(mesh):
    spread = ("grp", "rng")
    return jax.shard_map(
        local,
        mesh=mesh,
        in_specs=(
            P(spread, None), P(), P(), P(), P(),
            P(spread), P(spread, None), P(spread), P(spread, None),
        ),
        out_specs=P(spread, None),
        check_vma=False,
    )
```

```python
import jax
import jax.numpy as jnp
from jax import lax
from jax.experimental import pallas as pl
from jax.experimental.pallas import tpu as pltpu
from jax.sharding import PartitionSpec as P


TILE = 128
PORTAL = 64
MAXLONG = 6
EPSILON = 1e-06
LANES = 128
HEAD = 64
CHUNK = 64
BLOCK = 256
PICKS = 8
SLOTS = 15
RIM = SLOTS * PORTAL
FIRST = (1, 2, 3, 4, 5, 6, 7, 8, 9, 10, 14)
SECOND = (11, 15, 12, 13)
MIB = 1024 * 1024
SCALE2 = HEAD**-0.5 * 1.4426950408889634
F32 = jnp.float32
NEVER = float(jnp.finfo(jnp.bfloat16).min)
BF16 = jnp.bfloat16

VMEM = pl.BlockSpec(memory_space=pltpu.VMEM)
SMEM = pl.BlockSpec(memory_space=pltpu.SMEM)
HBM = pl.BlockSpec(memory_space=pltpu.HBM)


def region(x, y, c):
    return (x % 4) * 4 + (y % 2) * 2 + c % 2


def moved(dx, dy, dc):
    return [
        (region(x, y, c), region(x + dx, y + dy, c ^ dc))
        for x in range(4)
        for y in range(2)
        for c in range(2)
    ]


def place_of(index):
    return index // 4, (index // 2) % 2, index % 2


def normalized(features):
    widened = features.astype(F32)
    factor = lax.rsqrt(jnp.mean(widened * widened, axis=1, keepdims=True) + EPSILON)
    return (widened * factor).astype(BF16)


def norm_kernel(feat_ref, a_ref, up_ref, down_ref):
    rows = feat_ref.shape[0]
    normed = normalized(feat_ref[...])
    a_ref[...] = normed
    down_ref[...] = normed[:TILE]
    up_ref[...] = normed[rows - TILE :]


def pack_kernel(send_ref, a_ref, x1_ref, x2_ref, x3_ref, mate_ref, picks_ref):
    x, y, c = place_of(lax.axis_index("grp"))

    def pick(dx, dy, dc):
        return send_ref[0, ((x + dx) % 4) * 4 + (y ^ dy) * 2 + (c ^ dc)]

    def tile(index):
        return a_ref[pl.ds(pl.multiple_of(index * PORTAL, PORTAL), PORTAL)]

    for dx, ref in ((1, x1_ref), (2, x2_ref), (3, x3_ref)):
        for dc in range(2):
            ref[dc * PORTAL : (dc + 1) * PORTAL] = tile(pick(dx, 0, dc))
    mate_ref[...] = tile(pick(0, 0, 1))
    row = lax.broadcasted_iota(jnp.int32, picks_ref.shape, 0)
    picks = jnp.zeros(row.shape, jnp.int32)
    for i in range(PICKS):
        picks = jnp.where(row == i, pick(i // 2, 1, i % 2), picks)
    picks_ref[...] = picks.astype(F32).astype(BF16)


def relay_kernel(feat_ref, picks_ref, *refs):
    out_refs, normed_ref = refs[:-1], refs[-1]
    rows = feat_ref.shape[0]
    normed_ref[...] = normalized(feat_ref[...]).astype(F32)
    picks = picks_ref[...].astype(F32)
    for i, ref in enumerate(out_refs):
        pick = jnp.broadcast_to(picks[i : i + 1], (PORTAL, picks.shape[1]))
        tile = normed_ref[:PORTAL]
        for k in range(1, rows // PORTAL):
            tile = jnp.where(
                pick == float(k), normed_ref[k * PORTAL : (k + 1) * PORTAL], tile
            )
        ref[...] = tile.astype(BF16)


def dot(x, w):
    return jnp.dot(x, w, preferred_element_type=F32)


def block_cols(b):
    return slice(b * BLOCK, (b + 1) * BLOCK)


def low_lanes():
    return lax.broadcasted_iota(jnp.int32, (TILE, LANES), 1) < HEAD


def pair_queries(q):
    low = low_lanes()
    zero = jnp.zeros_like(q)
    return jnp.concatenate([jnp.where(low, q, zero), jnp.where(low, zero, q)], axis=0)


def unpair(x):
    return jnp.where(low_lanes(), x[:TILE], x[TILE:])


def set_eye(eye_ref):
    row = lax.broadcasted_iota(jnp.int32, eye_ref.shape, 0) % TILE
    lane = lax.broadcasted_iota(jnp.int32, eye_ref.shape, 1)
    eye_ref[...] = jnp.where(row == lane, 1.0, 0.0).astype(BF16)


def masked(keep):
    return jnp.where(keep, 0.0, NEVER).astype(BF16)


def pair_scores(q, eye, keys, mask):
    return lax.dot_general(
        jnp.concatenate([pair_queries(q), eye], axis=1),
        jnp.concatenate([keys, mask], axis=1),
        (((1,), (1,)), ((), ())),
        preferred_element_type=F32,
    )


def weigh(p, values):
    ones = jnp.ones(values.shape, BF16)
    both = dot(p, jnp.concatenate([values, ones], axis=1))
    return unpair(both[:, :LANES]), unpair(both[:, LANES:])


def chain(j, tiles):
    h, t = j // tiles, j % tiles
    return t, slice(t * TILE, (t + 1) * TILE), slice(h * LANES, (h + 1) * LANES)


def staged(count, fill, first, second, third):
    for j in range(count + 2):
        fill(j)
        if j < count:
            first(j)
        if 0 <= j - 1 < count:
            second(j - 1)
        if 0 <= j - 2:
            third(j - 2)


def spread_fill(parts, per_block):
    def fill(j):
        if j == 0:
            for part in parts:
                part(0)
        b, i = j // per_block + 1, j % per_block
        if i < len(parts):
            parts[i](b)

    return fill


def here_kernel(
    reach_ref, a_ref, wq_ref, wk_ref, wv_ref, q_ref, acc_ref, max_ref, sum_ref,
    k_s, v_s, eye_s, mask_s, s0, s1, p0, p1,
):
    rows, width = q_ref.shape
    tiles = rows // TILE
    blocks = width // BLOCK
    s_s, p_s = (s0, s1), (p0, p1)
    set_eye(eye_s)
    key = lax.broadcasted_iota(jnp.int32, (rows, LANES), 0)
    place = lax.broadcasted_iota(jnp.int32, (rows, LANES), 1)
    for t in range(tiles):
        mask_s[t * rows : (t + 1) * rows] = masked(jnp.abs(place + t * TILE - key) <= reach_ref[0])

    def project(w_ref, out_ref, scale=None):
        def part(b):
            if b < blocks:
                cols = block_cols(b)
                product = dot(a_ref[:rows], w_ref[:, cols])
                if scale is not None:
                    product = product * scale
                out_ref[:, cols] = product.astype(BF16)

        return part

    def first(j):
        t, here, cols = chain(j, tiles)
        mask = mask_s[t * rows : (t + 1) * rows]
        s_s[j % 2][...] = pair_scores(q_ref[here, cols], eye_s[...], k_s[:, cols], mask)

    def second(j):
        for r in range(0, 2 * TILE, CHUNK):
            s = s_s[j % 2][r : r + CHUNK]
            m = jnp.max(s, axis=1, keepdims=True)
            max_ref[j, r : r + CHUNK] = jnp.broadcast_to(m, (CHUNK, LANES))
            p_s[j % 2][r : r + CHUNK] = jnp.exp2(s - m).astype(BF16)

    def third(j):
        _, here, cols = chain(j, tiles)
        acc, total = weigh(p_s[j % 2][...], v_s[:, cols])
        acc_ref[here, cols] = acc
        sum_ref[here, cols] = total

    fill = spread_fill(
        [project(wq_ref, q_ref, SCALE2), project(wk_ref, k_s), project(wv_ref, v_s)],
        tiles * BLOCK // LANES,
    )
    staged(tiles * width // LANES, fill, first, second, third)


def tile_rows(pos):
    return slice((pos - 1) * PORTAL, pos * PORTAL)


def far_kernel(
    mine_ref, l1_ref, l4_ref, l5_ref, x1_ref, x2_ref, x3_ref, swap_ref, lo_ref, hi_ref,
    wk_ref, wv_ref, ke_ref, ve_ref, x_s,
):
    tiles = {8: mine_ref[...], 9: l1_ref[...], 10: l4_ref[...], 14: l5_ref[...]}
    for dx, ref in ((1, x1_ref), (2, x2_ref), (3, x3_ref)):
        tiles[2 * dx] = ref[:PORTAL]
    for i, pos in enumerate((1, 3, 5, 7)):
        tiles[pos] = swap_ref[i * PORTAL : (i + 1) * PORTAL]
    for i, pos in enumerate(FIRST):
        x_s[tile_rows(i + 1)] = tiles[pos]
    near = len(FIRST) * PORTAL
    x_s[near : near + TILE] = lo_ref[...]
    x_s[near + TILE :] = hi_ref[...]
    for b in range(wk_ref.shape[1] // BLOCK):
        cols = block_cols(b)
        for w_ref, out_ref in ((wk_ref, ke_ref), (wv_ref, ve_ref)):
            product = dot(x_s[...], w_ref[:, cols]).astype(BF16)
            for i, pos in enumerate(FIRST):
                out_ref[tile_rows(pos), cols] = product[tile_rows(i + 1)]
            out_ref[RIM:, cols] = product[near:]


def last_kernel(
    peers_hbm, count_hbm, reach_ref, q_ref, acc_ref, max_ref, sum_ref, feat_ref, ke_ref, ve_ref,
    l0, l1, l2, l3, wk_ref, wv_ref, wo_ref, out_hbm, k_ref, v_ref,
    x_s, att_s, kl_s, vl_s, eye_s, mask_s, keep0, keep1, s0, s1, p0, p1, out_s,
    peers_ref, count_ref, sems,
):
    rows, width = q_ref.shape
    tiles = rows // TILE
    blocks = width // BLOCK
    span = MAXLONG * PORTAL
    keys = span + TILE
    s_s, p_s, keep_s = (s0, s1), (p0, p1), (keep0, keep1)
    peers_copy = pltpu.make_async_copy(peers_hbm, peers_ref, sems.at[0])
    count_copy = pltpu.make_async_copy(count_hbm, count_ref, sems.at[1])
    peers_copy.start()
    count_copy.start()
    for i, ref in enumerate((l0, l1, l2, l3)):
        x_s[i * PORTAL : (i + 1) * PORTAL] = ref[...]
    x, y, c = place_of(lax.axis_index("grp"))
    set_eye(eye_s)
    near = lax.broadcasted_iota(jnp.int32, (TILE, LANES), 0)
    place = lax.broadcasted_iota(jnp.int32, (TILE, LANES), 1)
    slot = lax.broadcasted_iota(jnp.int32, (span, LANES), 0) // PORTAL
    for t in range(tiles):
        gap = place + TILE - near if t == 0 else near + TILE - place
        mask_s[t * keys + span : (t + 1) * keys] = masked(gap <= reach_ref[0])
    starts = []

    def lists():
        peers_copy.wait()
        count_copy.wait()
        for t in range(tiles):
            mask_s[t * keys : t * keys + span] = masked(slot < count_ref[t])
            for s in range(MAXLONG):
                px, py, pc = place_of(peers_ref[t, s])
                pos = (y ^ py) * 8 + ((x - px + 4) % 4) * 2 + (c ^ pc)
                starts.append(pl.multiple_of((pos - 1) * PORTAL, PORTAL))

    def project(w_ref, all_ref, listed_ref):
        def part(b):
            if b < blocks:
                cols = block_cols(b)
                product = dot(x_s[...], w_ref[:, cols]).astype(BF16)
                for i, pos in enumerate(SECOND):
                    all_ref[tile_rows(pos), cols] = product[tile_rows(i + 1)]
                if not starts:
                    lists()
                for t in range(tiles):
                    for s in range(MAXLONG):
                        row = t * keys + s * PORTAL
                        listed_ref[row : row + PORTAL, cols] = all_ref[
                            pl.ds(starts[t * MAXLONG + s], PORTAL), cols
                        ]
                    rim = RIM + t * TILE
                    listed_ref[t * keys + span : (t + 1) * keys, cols] = all_ref[
                        rim : rim + TILE, cols
                    ]

        return part

    def first(j):
        t, here, cols = chain(j, tiles)
        mine = slice(t * keys, (t + 1) * keys)
        s_s[j % 2][...] = pair_scores(q_ref[here, cols], eye_s[...], kl_s[mine, cols], mask_s[mine])

    def second(j):
        for r in range(0, 2 * TILE, CHUNK):
            s = s_s[j % 2][r : r + CHUNK]
            band_max = max_ref[j, r : r + CHUNK]
            m = jnp.maximum(jnp.max(s, axis=1, keepdims=True), band_max)
            keep_s[j % 2][r : r + CHUNK] = jnp.exp2(band_max - m)
            p = jnp.exp2(s - jnp.concatenate([m] * (keys // LANES), axis=1))
            p_s[j % 2][r : r + CHUNK] = p.astype(BF16)

    def third(j):
        t, here, cols = chain(j, tiles)
        acc, total = weigh(p_s[j % 2][...], vl_s[t * keys : (t + 1) * keys, cols])
        keep = unpair(keep_s[j % 2][...])
        acc = acc + keep * acc_ref[here, cols]
        total = total + keep * sum_ref[here, cols]
        att_s[here, cols] = (acc / total).astype(BF16)

    fill = spread_fill(
        [project(wk_ref, k_ref, kl_s), project(wv_ref, v_ref, vl_s)], tiles * BLOCK // LANES
    )
    staged(tiles * width // LANES, fill, first, second, third)
    copies = []
    for b in range(blocks):
        cols = block_cols(b)
        projected = dot(att_s[...], wo_ref[:, cols])
        out_s[:, cols] = (feat_ref[:, cols].astype(F32) + projected).astype(BF16)
        copies.append(
            pltpu.make_async_copy(out_s.at[:, cols], out_hbm.at[:, cols], sems.at[2 + b])
        )
        copies[-1].start()
    for copy in copies:
        copy.wait()


def named(kernel, **kw):
    def run(*args):
        return pl.pallas_call(kernel, **kw)(*args)

    return run


def shape(*dims, dtype=BF16):
    return jax.ShapeDtypeStruct(dims, dtype)


def params(mib):
    return pltpu.CompilerParams(vmem_limit_bytes=mib * MIB)


def local(
    features, query_weight, key_weight, value_weight, out_weight,
    band_reach, long_peers, long_count, send_tile,
):
    rows, width = features.shape
    ranks = lax.axis_size("rng")
    tall = shape(2 * PORTAL, width)
    half = shape(TILE, width)
    tile = shape(PORTAL, width)
    square = shape(rows, width)
    square = shape(rows, width)
    across = lax.ppermute(features, "grp", moved(0, 1, 0))
    a, up, down = named(
        norm_kernel,
        out_shape=(square, half, half),
        in_specs=[VMEM],
        out_specs=(VMEM,) * 3,
        compiler_params=params(4),
    )(features)
    x1, x2, x3, mate, picks = named(
        pack_kernel,
        out_shape=(tall, tall, tall, tile, shape(PICKS, width)),
        in_specs=[SMEM, VMEM],
        out_specs=(VMEM,) * 5,
        cost_estimate=pl.CostEstimate(flops=10**10, bytes_accessed=2**23, transcendentals=0),
        compiler_params=params(4),
    )(send_tile, a)
    x1, x2, x3 = [
        lax.ppermute(part, "grp", moved(dx, 0, 0))
        for dx, part in ((1, x1), (2, x2), (3, x3))
    ]
    picks = lax.ppermute(picks, "grp", moved(0, 1, 0))
    wide = shape(rows, width, dtype=F32)
    chains = rows // TILE * width // LANES
    tops = shape(chains, 2 * TILE, LANES, dtype=F32)

    def stages(keys):
        return [pltpu.VMEM((2 * TILE, keys), F32)] * 2 + [pltpu.VMEM((2 * TILE, keys), BF16)] * 2

    queries, acc, top, total = named(
        here_kernel,
        out_shape=(square, wide, tops, wide),
        in_specs=[SMEM] + [VMEM] * 4,
        out_specs=(VMEM,) * 4,
        scratch_shapes=[pltpu.VMEM((rows, width), BF16)] * 2
        + [pltpu.VMEM((2 * TILE, LANES), BF16), pltpu.VMEM((rows // TILE * rows, LANES), BF16)]
        + stages(rows),
        compiler_params=params(8),
    )(band_reach, a, query_weight, key_weight, value_weight)
    up, down, queries = lax.optimization_barrier((up, down, queries))
    lo = lax.ppermute(up, "rng", [(i, (i + 1) % ranks) for i in range(ranks)])
    hi = lax.ppermute(down, "rng", [(i, (i - 1) % ranks) for i in range(ranks)])
    relayed = named(
        relay_kernel,
        out_shape=(tile,) * PICKS,
        in_specs=[VMEM] * 2,
        out_specs=(VMEM,) * PICKS,
        scratch_shapes=[pltpu.VMEM((rows, width), F32)],
        compiler_params=params(4),
    )(across, picks)
    late = {i: lax.ppermute(relayed[i], "grp", moved(i // 2, 0, i % 2)) for i in range(1, PICKS)}
    swapped = lax.ppermute(
        jnp.concatenate([mate, x1[PORTAL:], x2[PORTAL:], x3[PORTAL:]], axis=0),
        "grp",
        moved(0, 0, 1),
    )
    far = shape(RIM + 2 * TILE, width)
    far_rows = len(FIRST) * PORTAL + 2 * TILE
    far_keys, far_values = named(
        far_kernel,
        out_shape=(far, far),
        in_specs=[VMEM] * 12,
        out_specs=(VMEM,) * 2,
        scratch_shapes=[pltpu.VMEM((far_rows, width), BF16)],
        compiler_params=params(8),
    )(
        relayed[0], late[1], late[2], late[6], x1, x2, x3, swapped, lo, hi,
        key_weight, value_weight,
    )
    span = MAXLONG * PORTAL + TILE
    listed = rows // TILE * span
    updated, _, _ = named(
        last_kernel,
        out_shape=(square, far, far),
        in_specs=[HBM, HBM, SMEM] + [VMEM] * (7 + len(SECOND) + 3),
        out_specs=(HBM, VMEM, VMEM),
        scratch_shapes=[
            pltpu.VMEM((len(SECOND) * PORTAL, width), BF16),
            pltpu.VMEM((rows, width), BF16),
            pltpu.VMEM((listed, width), BF16),
            pltpu.VMEM((listed, width), BF16),
            pltpu.VMEM((2 * TILE, LANES), BF16),
            pltpu.VMEM((listed, LANES), BF16),
            pltpu.VMEM((2 * TILE, LANES), F32),
            pltpu.VMEM((2 * TILE, LANES), F32),
        ]
        + stages(span)
        + [
            pltpu.VMEM((rows, width), BF16),
            pltpu.SMEM(long_peers.shape, jnp.int32),
            pltpu.SMEM(long_count.shape, jnp.int32),
            pltpu.SemaphoreType.DMA((2 + width // BLOCK,)),
        ],
        input_output_aliases={8: 1, 9: 2},
        compiler_params=params(14),
    )(
        long_peers, long_count, band_reach, queries, acc, top, total, features,
        far_keys, far_values, late[3], late[7], late[4], late[5], key_weight, value_weight, out_weight,
    )
    return updated


def solution(mesh):
    spread = ("grp", "rng")
    return jax.shard_map(
        local,
        mesh=mesh,
        in_specs=(
            P(spread, None), P(), P(), P(), P(),
            P(spread), P(spread, None), P(spread), P(spread, None),
        ),
        out_specs=P(spread, None),
        check_vma=False,
    )
```

```python
import jax
import jax.numpy as jnp
from jax import lax
from jax.experimental import pallas as pl
from jax.experimental.pallas import tpu as pltpu
from jax.sharding import PartitionSpec as P


TILE = 128
PORTAL = 64
MAXLONG = 6
EPSILON = 1e-06
LANES = 128
HEAD = 64
CHUNK = 64
BLOCK = 256
PICKS = 8
SLOTS = 15
RIM = SLOTS * PORTAL
FIRST = (1, 2, 3, 4, 5, 6, 7, 8, 9, 10, 14)
SECOND = (11, 15, 12, 13)
MIB = 1024 * 1024
SCALE2 = HEAD**-0.5 * 1.4426950408889634
F32 = jnp.float32
NEVER = float(jnp.finfo(jnp.bfloat16).min)
BF16 = jnp.bfloat16

VMEM = pl.BlockSpec(memory_space=pltpu.VMEM)
SMEM = pl.BlockSpec(memory_space=pltpu.SMEM)
HBM = pl.BlockSpec(memory_space=pltpu.HBM)


def region(x, y, c):
    return (x % 4) * 4 + (y % 2) * 2 + c % 2


def moved(dx, dy, dc):
    return [
        (region(x, y, c), region(x + dx, y + dy, c ^ dc))
        for x in range(4)
        for y in range(2)
        for c in range(2)
    ]


def place_of(index):
    return index // 4, (index // 2) % 2, index % 2


def normalized(features):
    widened = features.astype(F32)
    factor = lax.rsqrt(jnp.mean(widened * widened, axis=1, keepdims=True) + EPSILON)
    return (widened * factor).astype(BF16)


def norm_kernel(feat_ref, a_ref, up_ref, down_ref):
    rows = feat_ref.shape[0]
    normed = normalized(feat_ref[...])
    a_ref[...] = normed
    down_ref[...] = normed[:TILE]
    up_ref[...] = normed[rows - TILE :]


def pack_kernel(send_ref, a_ref, x1_ref, x2_ref, x3_ref, mate_ref, picks_ref):
    x, y, c = place_of(lax.axis_index("grp"))

    def pick(dx, dy, dc):
        return send_ref[0, ((x + dx) % 4) * 4 + (y ^ dy) * 2 + (c ^ dc)]

    def tile(index):
        return a_ref[pl.ds(pl.multiple_of(index * PORTAL, PORTAL), PORTAL)]

    for dx, ref in ((1, x1_ref), (2, x2_ref), (3, x3_ref)):
        for dc in range(2):
            ref[dc * PORTAL : (dc + 1) * PORTAL] = tile(pick(dx, 0, dc))
    mate_ref[...] = tile(pick(0, 0, 1))
    row = lax.broadcasted_iota(jnp.int32, picks_ref.shape, 0)
    picks = jnp.zeros(row.shape, jnp.int32)
    for i in range(PICKS):
        picks = jnp.where(row == i, pick(i // 2, 1, i % 2), picks)
    picks_ref[...] = picks.astype(F32).astype(BF16)


def relay_kernel(feat_ref, picks_ref, *refs):
    out_refs, normed_ref = refs[:-1], refs[-1]
    rows = feat_ref.shape[0]
    normed_ref[...] = normalized(feat_ref[...])
    picks = picks_ref[...]
    for i, ref in enumerate(out_refs):
        pick = jnp.broadcast_to(picks[i : i + 1], (PORTAL, picks.shape[1]))
        tile = normed_ref[:PORTAL]
        for k in range(1, rows // PORTAL):
            tile = jnp.where(
                pick == jnp.asarray(k, BF16), normed_ref[k * PORTAL : (k + 1) * PORTAL], tile
            )
        ref[...] = tile


def dot(x, w):
    return jnp.dot(x, w, preferred_element_type=F32)


def block_cols(b):
    return slice(b * BLOCK, (b + 1) * BLOCK)


def low_lanes():
    return lax.broadcasted_iota(jnp.int32, (TILE, LANES), 1) < HEAD


def pair_queries(q):
    low = low_lanes()
    zero = jnp.zeros_like(q)
    return jnp.concatenate([jnp.where(low, q, zero), jnp.where(low, zero, q)], axis=0)


def unpair(x):
    return jnp.where(low_lanes(), x[:TILE], x[TILE:])


def set_eye(eye_ref):
    row = lax.broadcasted_iota(jnp.int32, eye_ref.shape, 0) % TILE
    lane = lax.broadcasted_iota(jnp.int32, eye_ref.shape, 1)
    eye_ref[...] = jnp.where(row == lane, 1.0, 0.0).astype(BF16)


def masked(keep):
    return jnp.where(keep, 0.0, NEVER).astype(BF16)


def pair_scores(q, eye, keys, mask):
    return lax.dot_general(
        jnp.concatenate([pair_queries(q), eye], axis=1),
        jnp.concatenate([keys, mask], axis=1),
        (((1,), (1,)), ((), ())),
        preferred_element_type=F32,
    )


def weigh(p, values):
    ones = jnp.ones(values.shape, BF16)
    both = dot(p, jnp.concatenate([values, ones], axis=1))
    return unpair(both[:, :LANES]), unpair(both[:, LANES:])


def chain(j, tiles):
    h, t = j // tiles, j % tiles
    return t, slice(t * TILE, (t + 1) * TILE), slice(h * LANES, (h + 1) * LANES)


def staged(count, fill, first, second, third):
    for j in range(count + 2):
        fill(j)
        if j < count:
            first(j)
        if 0 <= j - 1 < count:
            second(j - 1)
        if 0 <= j - 2:
            third(j - 2)


def spread_fill(parts, per_block):
    def fill(j):
        if j == 0:
            for part in parts:
                part(0)
        b, i = j // per_block + 1, j % per_block
        if i < len(parts):
            parts[i](b)

    return fill


def here_kernel(
    reach_ref, a_ref, wq_ref, wk_ref, wv_ref, q_ref, acc_ref, max_ref, sum_ref,
    k_s, v_s, eye_s, mask_s, s0, s1, p0, p1,
):
    rows, width = q_ref.shape
    tiles = rows // TILE
    blocks = width // BLOCK
    s_s, p_s = (s0, s1), (p0, p1)
    set_eye(eye_s)
    key = lax.broadcasted_iota(jnp.int32, (rows, LANES), 0)
    place = lax.broadcasted_iota(jnp.int32, (rows, LANES), 1)
    for t in range(tiles):
        mask_s[t * rows : (t + 1) * rows] = masked(jnp.abs(place + t * TILE - key) <= reach_ref[0])

    def project(w_ref, out_ref, scale=None):
        def part(b):
            if b < blocks:
                cols = block_cols(b)
                product = dot(a_ref[:rows], w_ref[:, cols])
                if scale is not None:
                    product = product * scale
                out_ref[:, cols] = product.astype(BF16)

        return part

    def first(j):
        t, here, cols = chain(j, tiles)
        mask = mask_s[t * rows : (t + 1) * rows]
        s_s[j % 2][...] = pair_scores(q_ref[here, cols], eye_s[...], k_s[:, cols], mask)

    def second(j):
        for r in range(0, 2 * TILE, CHUNK):
            s = s_s[j % 2][r : r + CHUNK]
            m = jnp.max(s, axis=1, keepdims=True)
            max_ref[j, r : r + CHUNK] = jnp.broadcast_to(m, (CHUNK, LANES))
            p_s[j % 2][r : r + CHUNK] = jnp.exp2(s - m).astype(BF16)

    def third(j):
        _, here, cols = chain(j, tiles)
        acc, total = weigh(p_s[j % 2][...], v_s[:, cols])
        acc_ref[here, cols] = acc
        sum_ref[here, cols] = total

    fill = spread_fill(
        [project(wq_ref, q_ref, SCALE2), project(wk_ref, k_s), project(wv_ref, v_s)],
        tiles * BLOCK // LANES,
    )
    staged(tiles * width // LANES, fill, first, second, third)


def tile_rows(pos):
    return slice((pos - 1) * PORTAL, pos * PORTAL)


def far_kernel(
    mine_ref, l4_ref, l5_ref, x1_ref, x2_ref, x3_ref, swap_ref, lo_ref, hi_ref,
    wk_ref, wv_ref, ke_ref, ve_ref, x_s,
):
    tiles = {8: mine_ref[...], 10: l4_ref[...], 14: l5_ref[...]}
    for dx, ref in ((1, x1_ref), (2, x2_ref), (3, x3_ref)):
        tiles[2 * dx] = ref[:PORTAL]
    for i, pos in enumerate((1, 3, 5, 7, 9)):
        tiles[pos] = swap_ref[i * PORTAL : (i + 1) * PORTAL]
    for i, pos in enumerate(FIRST):
        x_s[tile_rows(i + 1)] = tiles[pos]
    near = len(FIRST) * PORTAL
    x_s[near : near + TILE] = lo_ref[...]
    x_s[near + TILE :] = hi_ref[...]
    for b in range(wk_ref.shape[1] // BLOCK):
        cols = block_cols(b)
        for w_ref, out_ref in ((wk_ref, ke_ref), (wv_ref, ve_ref)):
            product = dot(x_s[...], w_ref[:, cols]).astype(BF16)
            for i, pos in enumerate(FIRST):
                out_ref[tile_rows(pos), cols] = product[tile_rows(i + 1)]
            out_ref[RIM:, cols] = product[near:]


def last_kernel(
    peers_hbm, count_hbm, reach_ref, q_ref, acc_ref, max_ref, sum_ref, feat_ref, ke_ref, ve_ref,
    l0, l1, l2, l3, wk_ref, wv_ref, wo_ref, out_hbm, k_ref, v_ref,
    x_s, att_s, kl_s, vl_s, eye_s, mask_s, keep0, keep1, s0, s1, p0, p1, out_s,
    peers_ref, count_ref, sems,
):
    rows, width = q_ref.shape
    tiles = rows // TILE
    blocks = width // BLOCK
    span = MAXLONG * PORTAL
    keys = span + TILE
    s_s, p_s, keep_s = (s0, s1), (p0, p1), (keep0, keep1)
    peers_copy = pltpu.make_async_copy(peers_hbm, peers_ref, sems.at[0])
    count_copy = pltpu.make_async_copy(count_hbm, count_ref, sems.at[1])
    peers_copy.start()
    count_copy.start()
    for i, ref in enumerate((l0, l1, l2, l3)):
        x_s[i * PORTAL : (i + 1) * PORTAL] = ref[...]
    x, y, c = place_of(lax.axis_index("grp"))
    set_eye(eye_s)
    near = lax.broadcasted_iota(jnp.int32, (TILE, LANES), 0)
    place = lax.broadcasted_iota(jnp.int32, (TILE, LANES), 1)
    slot = lax.broadcasted_iota(jnp.int32, (span, LANES), 0) // PORTAL
    for t in range(tiles):
        gap = place + TILE - near if t == 0 else near + TILE - place
        mask_s[t * keys + span : (t + 1) * keys] = masked(gap <= reach_ref[0])
    starts = []

    def lists():
        peers_copy.wait()
        count_copy.wait()
        for t in range(tiles):
            mask_s[t * keys : t * keys + span] = masked(slot < count_ref[t])
            for s in range(MAXLONG):
                px, py, pc = place_of(peers_ref[t, s])
                pos = (y ^ py) * 8 + ((x - px + 4) % 4) * 2 + (c ^ pc)
                starts.append(pl.multiple_of((pos - 1) * PORTAL, PORTAL))

    def project(w_ref, all_ref, listed_ref):
        def part(b):
            if b < blocks:
                cols = block_cols(b)
                product = dot(x_s[...], w_ref[:, cols]).astype(BF16)
                for i, pos in enumerate(SECOND):
                    all_ref[tile_rows(pos), cols] = product[tile_rows(i + 1)]
                if not starts:
                    lists()
                for t in range(tiles):
                    for s in range(MAXLONG):
                        row = t * keys + s * PORTAL
                        listed_ref[row : row + PORTAL, cols] = all_ref[
                            pl.ds(starts[t * MAXLONG + s], PORTAL), cols
                        ]
                    rim = RIM + t * TILE
                    listed_ref[t * keys + span : (t + 1) * keys, cols] = all_ref[
                        rim : rim + TILE, cols
                    ]

        return part

    def first(j):
        t, here, cols = chain(j, tiles)
        mine = slice(t * keys, (t + 1) * keys)
        s_s[j % 2][...] = pair_scores(q_ref[here, cols], eye_s[...], kl_s[mine, cols], mask_s[mine])

    def second(j):
        for r in range(0, 2 * TILE, CHUNK):
            s = s_s[j % 2][r : r + CHUNK]
            band_max = max_ref[j, r : r + CHUNK]
            m = jnp.maximum(jnp.max(s, axis=1, keepdims=True), band_max)
            keep_s[j % 2][r : r + CHUNK] = jnp.exp2(band_max - m)
            p = jnp.exp2(s - jnp.concatenate([m] * (keys // LANES), axis=1))
            p_s[j % 2][r : r + CHUNK] = p.astype(BF16)

    def third(j):
        t, here, cols = chain(j, tiles)
        acc, total = weigh(p_s[j % 2][...], vl_s[t * keys : (t + 1) * keys, cols])
        keep = unpair(keep_s[j % 2][...])
        acc = acc + keep * acc_ref[here, cols]
        total = total + keep * sum_ref[here, cols]
        att_s[here, cols] = (acc / total).astype(BF16)

    fill = spread_fill(
        [project(wk_ref, k_ref, kl_s), project(wv_ref, v_ref, vl_s)], tiles * BLOCK // LANES
    )
    staged(tiles * width // LANES, fill, first, second, third)
    copies = []
    for b in range(blocks):
        cols = block_cols(b)
        projected = dot(att_s[...], wo_ref[:, cols])
        out_s[:, cols] = (feat_ref[:, cols].astype(F32) + projected).astype(BF16)
        copies.append(
            pltpu.make_async_copy(out_s.at[:, cols], out_hbm.at[:, cols], sems.at[2 + b])
        )
        copies[-1].start()
    for copy in copies:
        copy.wait()


def named(kernel, **kw):
    def run(*args):
        return pl.pallas_call(kernel, **kw)(*args)

    return run


def shape(*dims, dtype=BF16):
    return jax.ShapeDtypeStruct(dims, dtype)


def params(mib):
    return pltpu.CompilerParams(vmem_limit_bytes=mib * MIB)


def local(
    features, query_weight, key_weight, value_weight, out_weight,
    band_reach, long_peers, long_count, send_tile,
):
    rows, width = features.shape
    ranks = lax.axis_size("rng")
    tall = shape(2 * PORTAL, width)
    half = shape(TILE, width)
    tile = shape(PORTAL, width)
    square = shape(rows, width)
    square = shape(rows, width)
    across = lax.ppermute(features, "grp", moved(0, 1, 0))
    a, up, down = named(
        norm_kernel,
        out_shape=(square, half, half),
        in_specs=[VMEM],
        out_specs=(VMEM,) * 3,
        compiler_params=params(4),
    )(features)
    x1, x2, x3, mate, picks = named(
        pack_kernel,
        out_shape=(tall, tall, tall, tile, shape(PICKS, width)),
        in_specs=[SMEM, VMEM],
        out_specs=(VMEM,) * 5,
        cost_estimate=pl.CostEstimate(flops=10**10, bytes_accessed=2**23, transcendentals=0),
        compiler_params=params(4),
    )(send_tile, a)
    x1, x2, x3 = [
        lax.ppermute(part, "grp", moved(dx, 0, 0))
        for dx, part in ((1, x1), (2, x2), (3, x3))
    ]
    picks = lax.ppermute(picks, "grp", moved(0, 1, 0))
    wide = shape(rows, width, dtype=F32)
    chains = rows // TILE * width // LANES
    tops = shape(chains, 2 * TILE, LANES, dtype=F32)

    def stages(keys):
        return [pltpu.VMEM((2 * TILE, keys), F32)] * 2 + [pltpu.VMEM((2 * TILE, keys), BF16)] * 2

    queries, acc, top, total = named(
        here_kernel,
        out_shape=(square, wide, tops, wide),
        in_specs=[SMEM] + [VMEM] * 4,
        out_specs=(VMEM,) * 4,
        scratch_shapes=[pltpu.VMEM((rows, width), BF16)] * 2
        + [pltpu.VMEM((2 * TILE, LANES), BF16), pltpu.VMEM((rows // TILE * rows, LANES), BF16)]
        + stages(rows),
        compiler_params=params(8),
    )(band_reach, a, query_weight, key_weight, value_weight)
    up, down, queries = lax.optimization_barrier((up, down, queries))
    lo = lax.ppermute(up, "rng", [(i, (i + 1) % ranks) for i in range(ranks)])
    hi = lax.ppermute(down, "rng", [(i, (i - 1) % ranks) for i in range(ranks)])
    relayed = named(
        relay_kernel,
        out_shape=(tile,) * PICKS,
        in_specs=[VMEM] * 2,
        out_specs=(VMEM,) * PICKS,
        scratch_shapes=[pltpu.VMEM((rows, width), BF16)],
        compiler_params=params(4),
    )(across, picks)
    late = {i: lax.ppermute(relayed[i], "grp", moved(i // 2, 0, i % 2)) for i in range(2, PICKS)}
    swapped = lax.ppermute(
        jnp.concatenate([mate, x1[PORTAL:], x2[PORTAL:], x3[PORTAL:], relayed[1]], axis=0),
        "grp",
        moved(0, 0, 1),
    )
    far = shape(RIM + 2 * TILE, width)
    far_rows = len(FIRST) * PORTAL + 2 * TILE
    far_keys, far_values = named(
        far_kernel,
        out_shape=(far, far),
        in_specs=[VMEM] * 11,
        out_specs=(VMEM,) * 2,
        scratch_shapes=[pltpu.VMEM((far_rows, width), BF16)],
        compiler_params=params(8),
    )(
        relayed[0], late[2], late[6], x1, x2, x3, swapped, lo, hi,
        key_weight, value_weight,
    )
    span = MAXLONG * PORTAL + TILE
    listed = rows // TILE * span
    updated, _, _ = named(
        last_kernel,
        out_shape=(square, far, far),
        in_specs=[HBM, HBM, SMEM] + [VMEM] * (7 + len(SECOND) + 3),
        out_specs=(HBM, VMEM, VMEM),
        scratch_shapes=[
            pltpu.VMEM((len(SECOND) * PORTAL, width), BF16),
            pltpu.VMEM((rows, width), BF16),
            pltpu.VMEM((listed, width), BF16),
            pltpu.VMEM((listed, width), BF16),
            pltpu.VMEM((2 * TILE, LANES), BF16),
            pltpu.VMEM((listed, LANES), BF16),
            pltpu.VMEM((2 * TILE, LANES), F32),
            pltpu.VMEM((2 * TILE, LANES), F32),
        ]
        + stages(span)
        + [
            pltpu.VMEM((rows, width), BF16),
            pltpu.SMEM(long_peers.shape, jnp.int32),
            pltpu.SMEM(long_count.shape, jnp.int32),
            pltpu.SemaphoreType.DMA((2 + width // BLOCK,)),
        ],
        input_output_aliases={8: 1, 9: 2},
        compiler_params=params(14),
    )(
        long_peers, long_count, band_reach, queries, acc, top, total, features,
        far_keys, far_values, late[3], late[7], late[4], late[5], key_weight, value_weight, out_weight,
    )
    return updated


def solution(mesh):
    spread = ("grp", "rng")
    return jax.shard_map(
        local,
        mesh=mesh,
        in_specs=(
            P(spread, None), P(), P(), P(), P(),
            P(spread), P(spread, None), P(spread), P(spread, None),
        ),
        out_specs=P(spread, None),
        check_vma=False,
    )
```
